32 devices in a mesh: grp: 4 (over y, x), cp: 8 (over z, core).
Axes of the slice: x: 2, y: 2, z: 4, core: 2. Of those that a mesh axis runs over, the one named last changes fastest.
Arguments:
- queries: bfloat16 [16384, 2048], P(('grp', 'cp')), parts along dimension 0, may hold values from -6 to 6
- keys: bfloat16 [16384, 1024], P(('grp', 'cp')), parts along dimension 0, may hold values from -8 to 8
- values: bfloat16 [16384, 1024], P(('grp', 'cp')), parts along dimension 0, may hold values from -6 to 6
- doc_lengths: int32 [128], P('grp'), parts along dimension 0, may hold values from 1 to 1024, 4096 in all
Outputs:
- attended: bfloat16 [16384, 2048], P(('grp', 'cp')), parts along dimension 0
The draws below stay inside these ranges and needn't reach their ends.
There are 4 independent parts, one for each index of `grp`. The reference program is written for one: setup_inputs(seed, part) draws one part's arguments, and reference() takes and returns one part's arrays. A program takes and returns all parts, laid end to end along the dimension named above; each array names one. Nothing has to cross between parts.
Inputs may be any that keep to these rules, and one draw needn't show every extreme that they name: doc_lengths sums to 4096, and its largest entry is exactly 1024.
All inputs are finite; a program needn't handle non-finite values.
Results may differ from the reference program's by a relative error of at most 0.0031.
Values may be sent and summed in bfloat16 or wider, within the bound.
A program may use at most 64 MiB of HBM per device.

```python
import math
import jax
import jax.numpy as jnp
import numpy as np
from jax import lax

HQ = 16
HK = 8
DH = 128
TOK_DEV = 512
REACH = 2
TOKENS = 4096
MAXDOC = 1024
DOCS = 32


def draw_queries(key, part):
    drawn = jnp.clip(jax.random.normal(jax.random.fold_in(key, 11), (TOKENS, HQ * DH), jnp.float32), -6.0, 6.0)
    return drawn.astype(jnp.bfloat16)


def draw_keys(key, part):
    drawn = jnp.clip(jax.random.normal(jax.random.fold_in(key, 22), (TOKENS, HK * DH), jnp.float32), -6.0, 6.0)
    return drawn.astype(jnp.bfloat16)


def shard_levels(rng, extent, shards, low, largest):
    factor_of, own = 1.0, jax.random.fold_in(rng, 6)
    for dim, blocks in shards:
        draws = jnp.exp(jax.random.uniform(jax.random.fold_in(own, dim), (blocks,), jnp.float32, low / len(shards), largest / len(shards)))
        factor_of = factor_of * jnp.repeat(draws, extent[dim] // blocks).reshape([-1 if axis == dim else 1 for axis in range(len(extent))])
    return factor_of


def profile(count, total, bound, skew):
    weights = [(1 << 20) // math.isqrt(standing ** skew) + 1 for standing in range(2, count + 1)]
    surplus, given = total - bound - (count - 1), [1] * (count - 1)
    while surplus > 0:
        movable = [i for i in range(count - 1) if given[i] < bound]
        mass, remaining = sum([weights[i] for i in movable]), surplus
        for i in movable:
            extra = min(bound - given[i], max(1, remaining * weights[i] // mass), surplus)
            given[i] = given[i] + extra
            surplus = surplus - extra
    return np.array([bound] + given)


def ragged_sizes(key, number_of, total, most, skew):
    if number_of == 2:
        one = jax.random.randint(key, (), max(1, total - most), min(most, total - 1) + 1)
        return jnp.stack([one, total - one])
    lengths = jnp.asarray(profile(number_of, total, most, skew), jnp.int32)
    couples = (number_of - 1) // 2
    source_of, taker = lengths[1:1 + 2 * couples:2], lengths[2:2 + 2 * couples:2]
    room = jnp.minimum(source_of - 1, most - taker)
    passed = jax.random.randint(jax.random.fold_in(key, 1), (couples,), 0, 1 << 20) % (room + 1)
    lengths = lengths.at[1:1 + 2 * couples:2].set(source_of - passed).at[2:2 + 2 * couples:2].set(taker + passed)
    return lengths[jax.random.permutation(jax.random.fold_in(key, 2), number_of)]


def noise(rng, dims, spread, limit, shards=(), held_as=jnp.bfloat16):
    loudness = shard_levels(rng, dims, shards, -0.22, 0.18) if shards else 1.0
    array = jax.random.normal(rng, dims, jnp.float32) * spread * loudness
    return jnp.minimum(jnp.maximum(array, -limit), limit).astype(held_as)


def setup_inputs(seed: int = 0, part: int = 0) -> dict:
    arg_keys = jax.random.split(jax.random.key(seed), 5)
    part_splits = jax.random.split(jax.random.fold_in(arg_keys[4], part), 5)
    queries = draw_queries(jax.random.fold_in(jax.random.fold_in(arg_keys[4], part), 71), part)
    keys = draw_keys(jax.random.fold_in(jax.random.fold_in(arg_keys[4], part), 71), part)
    values = noise(part_splits[2], (TOKENS, HK * DH), 1.0, 6.0, ((0, 8),))
    doc_lengths = ragged_sizes(part_splits[3], DOCS, TOKENS, MAXDOC, 2).astype(jnp.int32)
    return {"queries": queries, "keys": keys, "values": values, "doc_lengths": doc_lengths}


query_scale = 144.0 ** -0.5


def doc_index(positions, doc_ends):
    return jnp.sum((positions[:, None] >= doc_ends[None, :]).astype(jnp.int32), axis=1).astype(jnp.int32)


def attend(query_rows, key_rows, value_rows, visible):
    tok_rows = query_rows.shape[0]
    key_count = key_rows.shape[0]
    groups = HQ // HK
    query_heads = query_rows.astype(jnp.float32).reshape(tok_rows, HK, groups, DH)
    key_heads = key_rows.astype(jnp.float32).reshape(key_count, HK, DH)
    value_heads = value_rows.astype(jnp.float32).reshape(key_count, HK, DH)
    scores = jnp.einsum("tkgd,wkd->kgtw", query_heads, key_heads) * query_scale
    scores = jnp.where(visible[None, None], scores, -jnp.inf)
    highest = jnp.max(scores, axis=-1, keepdims=True)
    weights = jnp.exp(scores - highest)
    totals = jnp.sum(weights, axis=-1)
    rounded = lax.optimization_barrier(weights.astype(jnp.bfloat16))
    mixed = jnp.einsum("kgtw,wkd->tkgd", rounded.astype(jnp.float32), value_heads)
    mixed = mixed / jnp.transpose(totals, (2, 0, 1))[..., None]
    return mixed.reshape(tok_rows, HQ * DH).astype(jnp.bfloat16)


def reference(queries, keys, values, doc_lengths):
    doc_ends = jnp.cumsum(doc_lengths).astype(jnp.int32)
    margin = REACH * TOK_DEV
    window = (REACH + 1) * TOK_DEV
    pad_keys = jnp.concatenate([jnp.zeros((margin, HK * DH), keys.dtype), keys], axis=0)
    pad_values = jnp.concatenate([jnp.zeros((margin, HK * DH), values.dtype), values], axis=0)

    def one_block(index):
        begin_row = (index * TOK_DEV).astype(jnp.int32)
        query_pos = begin_row + jnp.arange(TOK_DEV, dtype=jnp.int32)
        key_pos = begin_row - margin + jnp.arange(window, dtype=jnp.int32)
        same_doc = doc_index(query_pos, doc_ends)[:, None] == doc_index(key_pos, doc_ends)[None, :]
        visible = same_doc & (key_pos[None, :] <= query_pos[:, None]) & (key_pos[None, :] >= 0)
        query_rows = lax.dynamic_slice_in_dim(queries, begin_row, TOK_DEV, 0)
        key_rows = lax.dynamic_slice_in_dim(pad_keys, begin_row, window, 0)
        value_rows = lax.dynamic_slice_in_dim(pad_values, begin_row, window, 0)
        return attend(query_rows, key_rows, value_rows, visible)

    blocks = lax.map(one_block, jnp.arange(TOKENS // TOK_DEV, dtype=jnp.int32))
    return blocks.reshape(TOKENS, HQ * DH)
```

```python
import functools
import math

import jax
import jax.numpy as jnp
from jax import lax
from jax.experimental import pallas as pl
from jax.experimental.pallas import tpu as pltpu
from jax.sharding import PartitionSpec as P

HQ = 16
HK = 8
DH = 128
REACH = 2
GROUPS = HQ // HK
WIDTH = GROUPS * DH
TILE = 128
MASKED = -1e30

exponent_scale = 144.0 ** (-0.5) * math.log2(math.e)


def kernel(
    shards,
    lengths_ref,
    queries_ref,
    keys_ref,
    values_ref,
    out_ref,
    held,
    query_held,
    out_held,
    bias,
    load_sem,
    query_sem,
    out_sem,
    chip_send,
    chip_recv,
    core_send,
    core_recv,
):
    me = lax.axis_index("cp")
    core = lax.rem(me, 2)
    partner = me + 1 - 2 * core
    rows = keys_ref.shape[0]
    docs = lengths_ref.shape[0]
    window = REACH * rows + TILE
    own = pl.ds(REACH * rows, rows)
    near = pl.ds(rows, rows)
    far = pl.ds(0, rows)
    has_prev = me >= 2
    has_next = me < shards - 2

    def loads(head):
        lanes = pl.ds(pl.multiple_of(head * DH, DH), DH)
        return (
            pltpu.make_async_copy(keys_ref.at[:, lanes], held.at[head, 0, own], load_sem.at[head, 0]),
            pltpu.make_async_copy(values_ref.at[:, lanes], held.at[head, 1, own], load_sem.at[head, 1]),
        )

    def query_load(head):
        lanes = pl.ds(pl.multiple_of(head * WIDTH, WIDTH), WIDTH)
        return pltpu.make_async_copy(queries_ref.at[:, lanes], query_held.at[head], query_sem.at[head])

    def out_store(head):
        lanes = pl.ds(pl.multiple_of(head * WIDTH, WIDTH), WIDTH)
        return pltpu.make_async_copy(out_held.at[head], out_ref.at[:, lanes], out_sem.at[head])

    def to_next_chip(head):
        return pltpu.make_async_remote_copy(
            src_ref=held.at[head, :, own],
            dst_ref=held.at[head, :, far],
            send_sem=chip_send.at[head],
            recv_sem=chip_recv.at[head],
            device_id={"cp": me + 2},
            device_id_type=pl.DeviceIdType.MESH,
        )

    def to_partner(head, source):
        return pltpu.make_async_remote_copy(
            src_ref=held.at[head, :, source],
            dst_ref=held.at[head, :, near],
            send_sem=core_send.at[head],
            recv_sem=core_recv.at[head],
            device_id={"cp": partner},
            device_id_type=pl.DeviceIdType.MESH,
        )

    @pl.loop(0, HK)
    def _(head):
        for copy in loads(head):
            copy.start()

    barrier = pltpu.get_barrier_semaphore()
    pl.semaphore_signal(barrier, inc=1, device_id={"cp": partner}, device_id_type=pl.DeviceIdType.MESH)

    @pl.when(has_prev)
    def _():
        pl.semaphore_signal(barrier, inc=1, device_id={"cp": me - 2}, device_id_type=pl.DeviceIdType.MESH)

    @pl.when(has_next)
    def _():
        pl.semaphore_signal(barrier, inc=1, device_id={"cp": me + 2}, device_id_type=pl.DeviceIdType.MESH)

    peers = 1 + jnp.where(has_prev, 1, 0) + jnp.where(has_next, 1, 0)
    pl.semaphore_wait(barrier, peers)

    @pl.loop(0, HK)
    def _(head):
        for copy in loads(head):
            copy.wait()

        @pl.when(has_next)
        def _():
            to_next_chip(head).start()

        @pl.when(core == 0)
        def _():
            to_partner(head, own).start()

    @pl.loop(0, HK)
    def _(head):
        query_load(head).start()

    @pl.when(jnp.logical_not(has_prev))
    def _():
        held[:, :, far, :] = jnp.zeros((HK, 2, rows, DH), held.dtype)

    @pl.when(me == 0)
    def _():
        held[:, :, near, :] = jnp.zeros((HK, 2, rows, DH), held.dtype)

    for tile in range(rows // TILE):
        query_pos = me * rows + tile * TILE + lax.broadcasted_iota(jnp.int32, (TILE, 1), 0)

        def next_doc(doc, state):
            end, begins = state
            end = end + lengths_ref[doc]
            return end, jnp.maximum(begins, jnp.where(query_pos >= end, end, 0))

        _, begins = lax.fori_loop(0, docs, next_doc, (jnp.int32(0), jnp.zeros((TILE, 1), jnp.int32)))
        key_pos = (
            (me - REACH) * rows + tile * TILE + lax.broadcasted_iota(jnp.int32, (TILE, window), 1)
        )
        visible = (key_pos >= begins) & (key_pos <= query_pos)
        bias[pl.ds(tile * TILE, TILE), :] = jnp.where(visible, 0.0, MASKED)

    @pl.loop(0, HK)
    def _(head):
        query_load(head).wait()

        @pl.when(has_prev)
        def _():
            to_next_chip(head).wait_recv()

            @pl.when(core == 1)
            def _():
                to_partner(head, far).start()

        @pl.when(me >= 1)
        def _():
            to_partner(head, far).wait_recv()

        for tile in range(rows // TILE):
            span = pl.ds(tile * TILE, TILE)
            queries = query_held[head, span, :]
            stacked = jnp.concatenate(
                [queries[:, g * DH : (g + 1) * DH] for g in range(GROUPS)], axis=0
            )
            scores = lax.dot_general(
                stacked,
                held[head, 0, pl.ds(tile * TILE, window), :],
                (((1,), (1,)), ((), ())),
                preferred_element_type=jnp.float32,
            )
            scores = scores.reshape(GROUPS, TILE, window) * exponent_scale + bias[span, :][None]
            highest = jnp.max(scores, axis=-1, keepdims=True)
            weights = jnp.exp2(scores - highest)
            totals = jnp.sum(weights, axis=-1, keepdims=True)
            mixed = jnp.dot(
                weights.astype(jnp.bfloat16).reshape(GROUPS * TILE, window),
                held[head, 1, pl.ds(tile * TILE, window), :],
                preferred_element_type=jnp.float32,
            ).reshape(GROUPS, TILE, DH)
            mixed = (mixed / totals).astype(jnp.bfloat16)
            for g in range(GROUPS):
                out_held[head, span, pl.ds(g * DH, DH)] = mixed[g]
        out_store(head).start()

    @pl.loop(0, HK)
    def _(head):
        out_store(head).wait()

        @pl.when(has_next)
        def _():
            to_next_chip(head).wait_send()

        @pl.when(jnp.logical_or(core == 0, has_prev))
        def _():
            to_partner(head, far).wait_send()


def on_device(queries, keys, values, doc_lengths):
    rows = keys.shape[0]
    shards = lax.axis_size("cp")
    window = REACH * rows + TILE
    return pl.pallas_call(
        functools.partial(kernel, shards),
        out_shape=jax.ShapeDtypeStruct(queries.shape, queries.dtype),
        in_specs=[
            pl.BlockSpec(memory_space=pltpu.SMEM),
            pl.BlockSpec(memory_space=pl.ANY),
            pl.BlockSpec(memory_space=pl.ANY),
            pl.BlockSpec(memory_space=pl.ANY),
        ],
        out_specs=pl.BlockSpec(memory_space=pl.ANY),
        scratch_shapes=[
            pltpu.VMEM((HK, 2, (REACH + 1) * rows, DH), keys.dtype),
            pltpu.VMEM((HK, rows, WIDTH), queries.dtype),
            pltpu.VMEM((HK, rows, WIDTH), queries.dtype),
            pltpu.VMEM((rows, window), jnp.float32),
            pltpu.SemaphoreType.DMA((HK, 2)),
            pltpu.SemaphoreType.DMA((HK,)),
            pltpu.SemaphoreType.DMA((HK,)),
            pltpu.SemaphoreType.DMA((HK,)),
            pltpu.SemaphoreType.DMA((HK,)),
            pltpu.SemaphoreType.DMA((HK,)),
            pltpu.SemaphoreType.DMA((HK,)),
        ],
        compiler_params=pltpu.CompilerParams(
            collective_id=0, has_side_effects=True, vmem_limit_bytes=48 * 1024 * 1024
        ),
    )(doc_lengths, queries, keys, values)


def solution(mesh):
    return jax.shard_map(
        on_device,
        mesh=mesh,
        in_specs=(P(("grp", "cp"), None), P(("grp", "cp"), None), P(("grp", "cp"), None), P("grp")),
        out_specs=P(("grp", "cp"), None),
        check_vma=False,
    )
```

```python
import functools
import math

import jax
import jax.numpy as jnp
from jax import lax
from jax.experimental import pallas as pl
from jax.experimental.pallas import tpu as pltpu
from jax.sharding import PartitionSpec as P

HQ = 16
HK = 8
DH = 128
REACH = 2
GROUPS = HQ // HK
WIDTH = GROUPS * DH
TILE = 128
MASKED = -1e30

exponent_scale = 144.0 ** (-0.5) * math.log2(math.e)


LOG2E = math.log2(math.e)
SPLIT = HK // 2
MESH = pl.DeviceIdType.MESH


def kernel(
    shards,
    lengths_ref,
    queries_ref,
    keys_ref,
    values_ref,
    out_ref,
    held,
    query_held,
    out_held,
    query_back,
    slot,
    stat_out,
    stat_in,
    bias,
    back_bias,
    load_sem,
    query_sem,
    out_sem,
    core_send,
    core_recv,
    query_send,
    query_recv,
    slot_send,
    slot_recv,
    relay_send,
    relay_recv,
    stat_send,
    stat_recv,
):
    me = lax.axis_index("cp")
    core = lax.rem(me, 2)
    even = core == 0
    odd = core == 1
    partner = me + 1 - 2 * core
    rows = keys_ref.shape[0]
    docs = lengths_ref.shape[0]
    tiles = rows // TILE
    window = REACH * rows + TILE
    own = pl.ds(REACH * rows, rows)
    near = pl.ds(rows, rows)
    far = pl.ds(0, rows)
    has_prev = me >= 2
    has_next = me < shards - 2
    chip_begin = (me - core) * rows
    next_begin = chip_begin + 2 * rows

    def loads(head):
        lanes = pl.ds(pl.multiple_of(head * DH, DH), DH)
        return (
            pltpu.make_async_copy(keys_ref.at[:, lanes], held.at[head, 0, own], load_sem.at[head, 0]),
            pltpu.make_async_copy(values_ref.at[:, lanes], held.at[head, 1, own], load_sem.at[head, 1]),
        )

    def query_load(head):
        lanes = pl.ds(pl.multiple_of(head * WIDTH, WIDTH), WIDTH)
        return pltpu.make_async_copy(queries_ref.at[:, lanes], query_held.at[head], query_sem.at[head])

    def out_store(head):
        lanes = pl.ds(pl.multiple_of(head * WIDTH, WIDTH), WIDTH)
        return pltpu.make_async_copy(out_held.at[head], out_ref.at[:, lanes], out_sem.at[head])

    def remote(source, target, send, recv, device):
        return pltpu.make_async_remote_copy(
            src_ref=source,
            dst_ref=target,
            send_sem=send,
            recv_sem=recv,
            device_id={"cp": device},
            device_id_type=MESH,
        )

    def to_core(head, region):
        return remote(
            held.at[head, :, own], held.at[head, :, region], core_send.at[head], core_recv.at[head], partner
        )

    def query_to_prev(step, side):
        return remote(
            query_held.at[side * SPLIT + step],
            query_back.at[step],
            query_send.at[side * SPLIT + step],
            query_recv.at[step],
            me - 2 + side,
        )

    def slot_to_next(step, region):
        return remote(
            slot.at[step],
            held.at[core * SPLIT + step, :, region],
            slot_send.at[step],
            slot_recv.at[step],
            me + 2,
        )

    def relay(step, source, target):
        head = core * SPLIT + step
        return remote(
            held.at[head, :, source], held.at[head, :, target], relay_send.at[step], relay_recv.at[step], partner
        )

    def stat_to_next(step, head):
        return remote(
            stat_out.at[step], stat_in.at[head], stat_send.at[step], stat_recv.at[head], me + 2 - core
        )

    @pl.loop(0, SPLIT)
    def _(step):
        query_load(step).start()
        query_load(SPLIT + step).start()

    @pl.loop(0, HK)
    def _(head):
        for copy in loads(head):
            copy.start()

    barrier = pltpu.get_barrier_semaphore()

    def greet(device):
        pl.semaphore_signal(barrier, inc=1, device_id={"cp": device}, device_id_type=MESH)

    greet(partner)

    @pl.when(has_prev)
    def _():
        greet(me - 2)

        @pl.when(even)
        def _():
            greet(me - 1)

    @pl.when(has_next)
    def _():
        greet(me + 2)

        @pl.when(odd)
        def _():
            greet(me + 1)

    back_peers = jnp.where(has_prev, 2 - core, 0)
    next_peers = jnp.where(has_next, 1 + core, 0)
    pl.semaphore_wait(barrier, 1 + back_peers + next_peers)

    @pl.loop(0, SPLIT)
    def _(step):
        for side in range(2):
            query_load(side * SPLIT + step).wait()

            @pl.when(jnp.logical_and(even, has_prev))
            def _():
                query_to_prev(step, side).start()

    @pl.loop(0, HK)
    def _(head):
        for copy in loads(head):
            copy.wait()

        @pl.when(even)
        def _():
            to_core(head, near).start()

        @pl.when(jnp.logical_and(odd, head < SPLIT))
        def _():
            to_core(head, far).start()

    @pl.when(jnp.logical_not(has_prev))
    def _():
        @pl.when(even)
        def _():
            held[:, :, near, :] = jnp.zeros((HK, 2, rows, DH), held.dtype)
            stat_in[...] = jnp.full(stat_in.shape, MASKED, jnp.float32)

        @pl.when(odd)
        def _():
            held[:, :, far, :] = jnp.zeros((HK, 2, rows, DH), held.dtype)

    def doc_begins(positions):
        def next_doc(doc, state):
            end, begins = state
            end = end + lengths_ref[doc]
            return end, jnp.maximum(begins, jnp.where(positions >= end, end, 0))

        start = (jnp.int32(0), jnp.zeros(positions.shape, jnp.int32))
        return lax.fori_loop(0, docs, next_doc, start)[1]

    def sends_keys(boundary):
        positions = jnp.full((1, DH), boundary, jnp.int32)
        return boundary - doc_begins(positions) <= rows

    row_iota = lax.broadcasted_iota(jnp.int32, (TILE, 1), 0)
    floor = jnp.where(sends_keys(chip_begin), 0, chip_begin)[:, :1]
    for tile in range(tiles):
        query_pos = me * rows + tile * TILE + row_iota
        begins = jnp.maximum(doc_begins(query_pos), floor)
        first = jnp.where(even, (me - 1) * rows, (me - 2) * rows + tile * TILE)
        key_pos = first + lax.broadcasted_iota(jnp.int32, (TILE, window), 1)
        visible = (key_pos >= begins) & (key_pos <= query_pos)
        bias[pl.ds(tile * TILE, TILE), :] = jnp.where(visible, 0.0, MASKED)

    for tile in range(tiles):
        begins = doc_begins(next_begin + tile * TILE + row_iota)
        key_pos = chip_begin + lax.broadcasted_iota(jnp.int32, (TILE, 2 * rows), 1)
        back_bias[pl.ds(tile * TILE, TILE), :] = jnp.where(key_pos >= begins, 0.0, MASKED)

    next_keys = sends_keys(next_begin)
    diagonal = lax.broadcasted_iota(jnp.int32, (TILE, TILE), 0) == lax.broadcasted_iota(
        jnp.int32, (TILE, TILE), 1
    )

    def stack(queries):
        return jnp.concatenate([queries[:, g * DH : (g + 1) * DH] for g in range(GROUPS)], axis=0)

    def dot_keys(queries, keys):
        return lax.dot_general(
            queries, keys, (((1,), (1,)), ((), ())), preferred_element_type=jnp.float32
        )

    def softmax(scores, mask):
        scores = scores.reshape(GROUPS, TILE, scores.shape[-1]) * exponent_scale + mask[None]
        highest = jnp.max(scores, axis=-1, keepdims=True)
        weights = jnp.exp2(scores - highest)
        totals = jnp.sum(weights, axis=-1, keepdims=True)
        rounded = weights.astype(jnp.bfloat16).reshape(GROUPS * TILE, scores.shape[-1])
        return highest, totals, rounded

    def dot_values(weights, values):
        return jnp.dot(weights, values, preferred_element_type=jnp.float32)

    def attend_back(step):
        head = core * SPLIT + step
        older = pl.multiple_of((2 - core) * rows, TILE)
        newer = pl.multiple_of(2 * core * rows, TILE)
        newer_rows = pl.ds(newer, rows)
        for tile in range(tiles):
            span = pl.ds(tile * TILE, TILE)
            count = rows - tile * TILE
            older_rows = pl.ds(older + tile * TILE, count)
            queries = stack(query_back[step, span, :])
            scores = jnp.concatenate(
                [
                    dot_keys(queries, held[head, 0, older_rows, :]),
                    dot_keys(queries, held[head, 0, newer_rows, :]),
                ],
                axis=1,
            )
            highest, totals, weights = softmax(scores, back_bias[span, pl.ds(tile * TILE, count + rows)])
            mixed = dot_values(weights[:, :count], held[head, 1, older_rows, :]) + dot_values(
                weights[:, count:], held[head, 1, newer_rows, :]
            )
            mixed = mixed.reshape(GROUPS, TILE, DH) / totals
            level = highest + jnp.log(totals) * LOG2E
            sent = pl.ds(newer + tile * TILE, TILE)
            for g in range(GROUPS):
                kept = held[head, g, sent, :].astype(jnp.float32)
                slot[step, g, span, :] = jnp.where(next_keys, kept, mixed[g]).astype(jnp.bfloat16)
                row = jnp.sum(jnp.where(diagonal, level[g], 0.0), axis=0, keepdims=True)
                stat_out[step, pl.ds(tile * GROUPS + g, 1), :] = jnp.where(next_keys, MASKED, row)

    def attend_even(head):
        for tile in range(tiles):
            span = pl.ds(tile * TILE, TILE)
            count = rows + (tile + 1) * TILE
            keys = pl.ds(rows, count)
            scores = dot_keys(stack(query_held[head, span, :]), held[head, 0, keys, :])
            highest, totals, weights = softmax(scores, bias[span, pl.ds(0, count)])
            mixed = dot_values(weights, held[head, 1, keys, :]).reshape(GROUPS, TILE, DH)
            for g in range(GROUPS):
                row = stat_in[head, pl.ds(tile * GROUPS + g, 1), :]
                level = jnp.sum(jnp.where(diagonal, row, 0.0), axis=1, keepdims=True)
                top = jnp.maximum(highest[g], level)
                here = jnp.exp2(highest[g] - top)
                there = jnp.exp2(level - top)
                partial = held[head, g, pl.ds(rows + tile * TILE, TILE), :].astype(jnp.float32)
                both = (mixed[g] * here + partial * there) / (totals[g] * here + there)
                out_held[head, span, pl.ds(g * DH, DH)] = both.astype(jnp.bfloat16)

    def attend_odd(head):
        for tile in range(tiles):
            span = pl.ds(tile * TILE, TILE)
            keys = pl.ds(tile * TILE, window)
            scores = dot_keys(stack(query_held[head, span, :]), held[head, 0, keys, :])
            _, totals, weights = softmax(scores, bias[span, :])
            mixed = dot_values(weights, held[head, 1, keys, :]).reshape(GROUPS, TILE, DH)
            mixed = (mixed / totals).astype(jnp.bfloat16)
            for g in range(GROUPS):
                out_held[head, span, pl.ds(g * DH, DH)] = mixed[g]

    @pl.when(even)
    def _():
        @pl.loop(0, SPLIT)
        def _(head):
            to_core(head, far).wait_recv()

    @pl.when(odd)
    def _():
        @pl.loop(0, HK)
        def _(head):
            to_core(head, near).wait_recv()

    @pl.loop(0, SPLIT + 1)
    def _(turn):
        @pl.when(jnp.logical_and(has_next, turn < SPLIT))
        def _():
            query_to_prev(turn, 0).wait_recv()
            attend_back(turn)

            @pl.when(even)
            def _():
                slot_to_next(turn, near).start()

            @pl.when(odd)
            def _():
                slot_to_next(turn, far).start()

            stat_to_next(turn, core * SPLIT + turn).start()

        @pl.when(turn >= 1)
        def _():
            step = turn - 1

            @pl.when(has_prev)
            def _():
                slot_to_next(step, far).wait_recv()

                @pl.when(even)
                def _():
                    relay(step, near, far).start()

                @pl.when(odd)
                def _():
                    relay(step, far, near).start()

            @pl.loop(0, 2)
            def _(turn_side):
                side = lax.rem(core + turn_side, 2)
                head = side * SPLIT + step

                @pl.when(jnp.logical_and(has_prev, turn_side == 1))
                def _():
                    relay(step, near, far).wait_recv()

                @pl.when(even)
                def _():
                    @pl.when(has_prev)
                    def _():
                        stat_to_next(step, head).wait_recv()

                    attend_even(head)

                @pl.when(odd)
                def _():
                    attend_odd(head)

                out_store(head).start()

    @pl.loop(0, HK)
    def _(head):
        out_store(head).wait()

        @pl.when(jnp.logical_or(even, head < SPLIT))
        def _():
            to_core(head, near).wait_send()

    @pl.loop(0, SPLIT)
    def _(step):
        @pl.when(has_next)
        def _():
            slot_to_next(step, near).wait_send()
            stat_to_next(step, step).wait_send()

        @pl.when(has_prev)
        def _():
            relay(step, near, far).wait_send()

            @pl.when(even)
            def _():
                for side in range(2):
                    query_to_prev(step, side).wait_send()


def on_device(queries, keys, values, doc_lengths):
    rows = keys.shape[0]
    shards = lax.axis_size("cp")
    window = REACH * rows + TILE
    stats = rows // TILE * GROUPS
    dma = pltpu.SemaphoreType.DMA
    return pl.pallas_call(
        functools.partial(kernel, shards),
        out_shape=jax.ShapeDtypeStruct(queries.shape, queries.dtype),
        in_specs=[
            pl.BlockSpec(memory_space=pltpu.SMEM),
            pl.BlockSpec(memory_space=pl.ANY),
            pl.BlockSpec(memory_space=pl.ANY),
            pl.BlockSpec(memory_space=pl.ANY),
        ],
        out_specs=pl.BlockSpec(memory_space=pl.ANY),
        scratch_shapes=[
            pltpu.VMEM((HK, 2, (REACH + 1) * rows, DH), keys.dtype),
            pltpu.VMEM((HK, rows, WIDTH), queries.dtype),
            pltpu.VMEM((HK, rows, WIDTH), queries.dtype),
            pltpu.VMEM((SPLIT, rows, WIDTH), queries.dtype),
            pltpu.VMEM((SPLIT, 2, rows, DH), keys.dtype),
            pltpu.VMEM((SPLIT, stats, TILE), jnp.float32),
            pltpu.VMEM((HK, stats, TILE), jnp.float32),
            pltpu.VMEM((rows, window), jnp.float32),
            pltpu.VMEM((rows, REACH * rows), jnp.float32),
            dma((HK, 2)),
            dma((HK,)),
            dma((HK,)),
            dma((HK,)),
            dma((HK,)),
            dma((HK,)),
            dma((SPLIT,)),
            dma((SPLIT,)),
            dma((SPLIT,)),
            dma((SPLIT,)),
            dma((SPLIT,)),
            dma((SPLIT,)),
            dma((HK,)),
        ],
        compiler_params=pltpu.CompilerParams(
            collective_id=0, has_side_effects=True, vmem_limit_bytes=58 * 1024 * 1024
        ),
    )(doc_lengths, queries, keys, values)


def solution(mesh):
    return jax.shard_map(
        on_device,
        mesh=mesh,
        in_specs=(P(("grp", "cp"), None), P(("grp", "cp"), None), P(("grp", "cp"), None), P("grp")),
        out_specs=P(("grp", "cp"), None),
        check_vma=False,
    )
```

```python
import functools
import math

import jax
import jax.numpy as jnp
from jax import lax
from jax.experimental import pallas as pl
from jax.experimental.pallas import tpu as pltpu
from jax.sharding import PartitionSpec as P

HQ = 16
HK = 8
DH = 128
REACH = 2
GROUPS = HQ // HK
WIDTH = GROUPS * DH
TILE = 128
MASKED = -1e30

exponent_scale = 144.0 ** (-0.5) * math.log2(math.e)


LOG2E = math.log2(math.e)
SPLIT = HK // 2
MESH = pl.DeviceIdType.MESH


def kernel(
    shards,
    lengths_ref,
    queries_ref,
    keys_ref,
    values_ref,
    out_ref,
    held,
    query_held,
    out_held,
    query_back,
    slot,
    stat_out,
    stat_in,
    bias,
    back_bias,
    mixed_held,
    highest_held,
    totals_held,
    load_sem,
    query_sem,
    out_sem,
    core_send,
    core_recv,
    query_send,
    query_recv,
    slot_send,
    slot_recv,
    relay_send,
    relay_recv,
    stat_send,
    stat_recv,
):
    me = lax.axis_index("cp")
    core = lax.rem(me, 2)
    even = core == 0
    odd = core == 1
    partner = me + 1 - 2 * core
    rows = keys_ref.shape[0]
    docs = lengths_ref.shape[0]
    tiles = rows // TILE
    window = REACH * rows + TILE
    own = pl.ds(REACH * rows, rows)
    near = pl.ds(rows, rows)
    far = pl.ds(0, rows)
    has_prev = me >= 2
    has_next = me < shards - 2
    chip_begin = (me - core) * rows
    next_begin = chip_begin + 2 * rows

    def loads(head):
        lanes = pl.ds(pl.multiple_of(head * DH, DH), DH)
        return (
            pltpu.make_async_copy(keys_ref.at[:, lanes], held.at[head, 0, own], load_sem.at[head, 0]),
            pltpu.make_async_copy(values_ref.at[:, lanes], held.at[head, 1, own], load_sem.at[head, 1]),
        )

    def query_load(head):
        lanes = pl.ds(pl.multiple_of(head * WIDTH, WIDTH), WIDTH)
        return pltpu.make_async_copy(queries_ref.at[:, lanes], query_held.at[head], query_sem.at[head])

    def out_store(head):
        lanes = pl.ds(pl.multiple_of(head * WIDTH, WIDTH), WIDTH)
        return pltpu.make_async_copy(out_held.at[head], out_ref.at[:, lanes], out_sem.at[head])

    def remote(source, target, send, recv, device):
        return pltpu.make_async_remote_copy(
            src_ref=source,
            dst_ref=target,
            send_sem=send,
            recv_sem=recv,
            device_id={"cp": device},
            device_id_type=MESH,
        )

    def to_core(head, region):
        return remote(
            held.at[head, :, own], held.at[head, :, region], core_send.at[head], core_recv.at[head], partner
        )

    def query_to_prev(step, side):
        return remote(
            query_held.at[side * SPLIT + step],
            query_back.at[step],
            query_send.at[side * SPLIT + step],
            query_recv.at[step],
            me - 2 + side,
        )

    def slot_to_next(step, region):
        return remote(
            slot.at[step],
            held.at[core * SPLIT + step, :, region],
            slot_send.at[step],
            slot_recv.at[step],
            me + 2,
        )

    def relay(step, source, target):
        head = core * SPLIT + step
        return remote(
            held.at[head, :, source], held.at[head, :, target], relay_send.at[step], relay_recv.at[step], partner
        )

    def stat_to_next(step, head):
        return remote(
            stat_out.at[step], stat_in.at[head], stat_send.at[step], stat_recv.at[head], me + 2 - core
        )

    @pl.loop(0, SPLIT)
    def _(step):
        query_load(step).start()
        query_load(SPLIT + step).start()

    @pl.loop(0, HK)
    def _(head):
        for copy in loads(head):
            copy.start()

    barrier = pltpu.get_barrier_semaphore()

    def greet(device):
        pl.semaphore_signal(barrier, inc=1, device_id={"cp": device}, device_id_type=MESH)

    greet(partner)

    @pl.when(has_prev)
    def _():
        greet(me - 2)

        @pl.when(even)
        def _():
            greet(me - 1)

    @pl.when(has_next)
    def _():
        greet(me + 2)

        @pl.when(odd)
        def _():
            greet(me + 1)

    back_peers = jnp.where(has_prev, 2 - core, 0)
    next_peers = jnp.where(has_next, 1 + core, 0)
    pl.semaphore_wait(barrier, 1 + back_peers + next_peers)

    @pl.loop(0, SPLIT)
    def _(step):
        for side in range(2):
            query_load(side * SPLIT + step).wait()

            @pl.when(jnp.logical_and(even, has_prev))
            def _():
                query_to_prev(step, side).start()

    @pl.loop(0, HK)
    def _(head):
        for copy in loads(head):
            copy.wait()

        @pl.when(even)
        def _():
            to_core(head, near).start()

        @pl.when(jnp.logical_and(odd, head < SPLIT))
        def _():
            to_core(head, far).start()

    @pl.when(jnp.logical_not(has_prev))
    def _():
        @pl.when(even)
        def _():
            held[:, :, near, :] = jnp.zeros((HK, 2, rows, DH), held.dtype)
            stat_in[...] = jnp.full(stat_in.shape, MASKED, jnp.float32)

        @pl.when(odd)
        def _():
            held[:, :, far, :] = jnp.zeros((HK, 2, rows, DH), held.dtype)

    def doc_begins(positions):
        def next_doc(doc, state):
            end, begins = state
            end = end + lengths_ref[doc]
            return end, jnp.maximum(begins, jnp.where(positions >= end, end, 0))

        start = (jnp.int32(0), jnp.zeros(positions.shape, jnp.int32))
        return lax.fori_loop(0, docs, next_doc, start)[1]

    def sends_keys(boundary):
        positions = jnp.full((1, DH), boundary, jnp.int32)
        return boundary - doc_begins(positions) <= rows

    row_iota = lax.broadcasted_iota(jnp.int32, (TILE, 1), 0)
    floor = jnp.where(sends_keys(chip_begin), 0, chip_begin)[:, :1]
    for tile in range(tiles):
        query_pos = me * rows + tile * TILE + row_iota
        begins = jnp.maximum(doc_begins(query_pos), floor)
        first = jnp.where(even, (me - 1) * rows, (me - 2) * rows + tile * TILE)
        key_pos = first + lax.broadcasted_iota(jnp.int32, (TILE, window), 1)
        visible = (key_pos >= begins) & (key_pos <= query_pos)
        bias[pl.ds(tile * TILE, TILE), :] = jnp.where(visible, 0.0, MASKED)

    for tile in range(tiles):
        begins = doc_begins(next_begin + tile * TILE + row_iota)
        key_pos = chip_begin + lax.broadcasted_iota(jnp.int32, (TILE, 2 * rows), 1)
        back_bias[pl.ds(tile * TILE, TILE), :] = jnp.where(key_pos >= begins, 0.0, MASKED)

    next_keys = sends_keys(next_begin)
    diagonal = lax.broadcasted_iota(jnp.int32, (TILE, TILE), 0) == lax.broadcasted_iota(
        jnp.int32, (TILE, TILE), 1
    )

    def stack(queries):
        return jnp.concatenate([queries[:, g * DH : (g + 1) * DH] for g in range(GROUPS)], axis=0)

    def dot_keys(queries, keys):
        return lax.dot_general(
            queries, keys, (((1,), (1,)), ((), ())), preferred_element_type=jnp.float32
        )

    def softmax(scores, mask):
        scores = scores.reshape(GROUPS, TILE, scores.shape[-1]) * exponent_scale + mask[None]
        highest = jnp.max(scores, axis=-1, keepdims=True)
        weights = jnp.exp2(scores - highest)
        totals = jnp.sum(weights, axis=-1, keepdims=True)
        rounded = weights.astype(jnp.bfloat16).reshape(GROUPS * TILE, scores.shape[-1])
        return highest, totals, rounded

    def dot_values(weights, values):
        return jnp.dot(weights, values, preferred_element_type=jnp.float32)

    def attend_back(step):
        head = core * SPLIT + step
        older = pl.multiple_of((2 - core) * rows, TILE)
        newer = pl.multiple_of(2 * core * rows, TILE)
        newer_rows = pl.ds(newer, rows)
        for tile in range(tiles):
            span = pl.ds(tile * TILE, TILE)
            count = rows - tile * TILE
            older_rows = pl.ds(older + tile * TILE, count)
            queries = stack(query_back[step, span, :])
            scores = jnp.concatenate(
                [
                    dot_keys(queries, held[head, 0, older_rows, :]),
                    dot_keys(queries, held[head, 0, newer_rows, :]),
                ],
                axis=1,
            )
            highest, totals, weights = softmax(scores, back_bias[span, pl.ds(tile * TILE, count + rows)])
            mixed = dot_values(weights[:, :count], held[head, 1, older_rows, :]) + dot_values(
                weights[:, count:], held[head, 1, newer_rows, :]
            )
            mixed = mixed.reshape(GROUPS, TILE, DH) / totals
            level = highest + jnp.log(totals) * LOG2E
            sent = pl.ds(newer + tile * TILE, TILE)
            for g in range(GROUPS):
                kept = held[head, g, sent, :].astype(jnp.float32)
                slot[step, g, span, :] = jnp.where(next_keys, kept, mixed[g]).astype(jnp.bfloat16)
                row = jnp.sum(jnp.where(diagonal, level[g], 0.0), axis=0, keepdims=True)
                stat_out[step, pl.ds(tile * GROUPS + g, 1), :] = jnp.where(next_keys, MASKED, row)

    def attend_even(head):
        for tile in range(tiles):
            span = pl.ds(tile * TILE, TILE)
            count = rows + (tile + 1) * TILE
            keys = pl.ds(rows, count)
            scores = dot_keys(stack(query_held[head, span, :]), held[head, 0, keys, :])
            highest, totals, weights = softmax(scores, bias[span, pl.ds(0, count)])
            mixed = dot_values(weights, held[head, 1, keys, :]).reshape(GROUPS, TILE, DH)
            for g in range(GROUPS):
                row = stat_in[head, pl.ds(tile * GROUPS + g, 1), :]
                level = jnp.sum(jnp.where(diagonal, row, 0.0), axis=1, keepdims=True)
                top = jnp.maximum(highest[g], level)
                here = jnp.exp2(highest[g] - top)
                there = jnp.exp2(level - top)
                partial = held[head, g, pl.ds(rows + tile * TILE, TILE), :].astype(jnp.float32)
                both = (mixed[g] * here + partial * there) / (totals[g] * here + there)
                out_held[head, span, pl.ds(g * DH, DH)] = both.astype(jnp.bfloat16)

    def attend_near(head):
        for tile in range(tiles):
            span = pl.ds(tile * TILE, TILE)
            skipped = rows - tile * TILE
            count = window - skipped
            keys = pl.ds(rows, count)
            scores = dot_keys(stack(query_held[head, span, :]), held[head, 0, keys, :])
            highest, totals, weights = softmax(scores, bias[span, pl.ds(skipped, count)])
            mixed = dot_values(weights, held[head, 1, keys, :]).reshape(GROUPS, TILE, DH)
            mixed_held[head, :, span, :] = mixed
            highest_held[head, :, span, :] = jnp.broadcast_to(highest, (GROUPS, TILE, DH))
            totals_held[head, :, span, :] = jnp.broadcast_to(totals, (GROUPS, TILE, DH))

    def attend_far(head):
        for tile in range(tiles):
            span = pl.ds(tile * TILE, TILE)
            count = rows - tile * TILE
            keys = pl.ds(tile * TILE, count)
            scores = dot_keys(stack(query_held[head, span, :]), held[head, 0, keys, :])
            highest, totals, weights = softmax(scores, bias[span, pl.ds(0, count)])
            mixed = dot_values(weights, held[head, 1, keys, :]).reshape(GROUPS, TILE, DH)
            earlier = highest_held[head, :, span, :]
            top = jnp.maximum(highest, earlier)
            here = jnp.exp2(highest - top)
            there = jnp.exp2(earlier - top)
            mixed = mixed * here + mixed_held[head, :, span, :] * there
            mixed = mixed / (totals * here + totals_held[head, :, span, :] * there)
            for g in range(GROUPS):
                out_held[head, span, pl.ds(g * DH, DH)] = mixed[g].astype(jnp.bfloat16)

    def attend_last(head):
        @pl.when(even)
        def _():
            @pl.when(has_prev)
            def _():
                stat_to_next(0, head).wait_recv()

            attend_even(head)

        @pl.when(odd)
        def _():
            attend_far(head)

        out_store(head).start()

    @pl.when(even)
    def _():
        @pl.loop(0, SPLIT)
        def _(head):
            to_core(head, far).wait_recv()

    @pl.when(odd)
    def _():
        @pl.loop(0, HK)
        def _(head):
            to_core(head, near).wait_recv()

    @pl.loop(0, HK + SPLIT + 2)
    def _(count):
        turn = count - 2
        step = turn - 1

        @pl.when(jnp.logical_and(has_next, jnp.logical_and(turn >= 0, turn < SPLIT)))
        def _():
            query_to_prev(turn, 0).wait_recv()
            attend_back(turn)

            @pl.when(even)
            def _():
                slot_to_next(turn, near).start()

            @pl.when(odd)
            def _():
                slot_to_next(turn, far).start()

            stat_to_next(turn, core * SPLIT + turn).start()

        @pl.when(jnp.logical_and(has_prev, jnp.logical_and(step >= 0, step < SPLIT)))
        def _():
            slot_to_next(step, far).wait_recv()

            @pl.when(even)
            def _():
                relay(step, near, far).start()

            @pl.when(odd)
            def _():
                relay(step, far, near).start()

        @pl.when(jnp.logical_and(odd, count < HK))
        def _():
            attend_near(count)

        done = count - 3 - core * (SPLIT - 1)

        @pl.when(jnp.logical_and(done >= 0, done < HK))
        def _():
            relayed = lax.div(done, SPLIT)
            step = lax.rem(done, SPLIT)

            @pl.when(jnp.logical_and(has_prev, relayed == 1))
            def _():
                relay(step, near, far).wait_recv()

            attend_last(lax.rem(core + relayed, 2) * SPLIT + step)

    @pl.loop(0, HK)
    def _(head):
        out_store(head).wait()

        @pl.when(jnp.logical_or(even, head < SPLIT))
        def _():
            to_core(head, near).wait_send()

    @pl.loop(0, SPLIT)
    def _(step):
        @pl.when(has_next)
        def _():
            slot_to_next(step, near).wait_send()
            stat_to_next(step, step).wait_send()

        @pl.when(has_prev)
        def _():
            relay(step, near, far).wait_send()

            @pl.when(even)
            def _():
                for side in range(2):
                    query_to_prev(step, side).wait_send()


def on_device(queries, keys, values, doc_lengths):
    rows = keys.shape[0]
    shards = lax.axis_size("cp")
    window = REACH * rows + TILE
    stats = rows // TILE * GROUPS
    dma = pltpu.SemaphoreType.DMA
    return pl.pallas_call(
        functools.partial(kernel, shards),
        out_shape=jax.ShapeDtypeStruct(queries.shape, queries.dtype),
        in_specs=[
            pl.BlockSpec(memory_space=pltpu.SMEM),
            pl.BlockSpec(memory_space=pltpu.HBM),
            pl.BlockSpec(memory_space=pltpu.HBM),
            pl.BlockSpec(memory_space=pltpu.HBM),
        ],
        out_specs=pl.BlockSpec(memory_space=pl.ANY),
        scratch_shapes=[
            pltpu.VMEM((HK, 2, (REACH + 1) * rows, DH), keys.dtype),
            pltpu.VMEM((HK, rows, WIDTH), queries.dtype),
            pltpu.VMEM((HK, rows, WIDTH), queries.dtype),
            pltpu.VMEM((SPLIT, rows, WIDTH), queries.dtype),
            pltpu.VMEM((SPLIT, 2, rows, DH), keys.dtype),
            pltpu.VMEM((SPLIT, stats, TILE), jnp.float32),
            pltpu.VMEM((HK, stats, TILE), jnp.float32),
            pltpu.VMEM((rows, window), jnp.float32),
            pltpu.VMEM((rows, REACH * rows), jnp.float32),
            pltpu.VMEM((HK, GROUPS, rows, DH), jnp.float32),
            pltpu.VMEM((HK, GROUPS, rows, DH), jnp.float32),
            pltpu.VMEM((HK, GROUPS, rows, DH), jnp.float32),
            dma((HK, 2)),
            dma((HK,)),
            dma((HK,)),
            dma((HK,)),
            dma((HK,)),
            dma((HK,)),
            dma((SPLIT,)),
            dma((SPLIT,)),
            dma((SPLIT,)),
            dma((SPLIT,)),
            dma((SPLIT,)),
            dma((SPLIT,)),
            dma((HK,)),
        ],
        compiler_params=pltpu.CompilerParams(
            collective_id=0, has_side_effects=True, vmem_limit_bytes=58 * 1024 * 1024
        ),
    )(doc_lengths, queries, keys, values)


def solution(mesh):
    return jax.shard_map(
        on_device,
        mesh=mesh,
        in_specs=(P(("grp", "cp"), None), P(("grp", "cp"), None), P(("grp", "cp"), None), P("grp")),
        out_specs=P(("grp", "cp"), None),
        check_vma=False,
    )
```

```python
import functools
import math

import jax
import jax.numpy as jnp
from jax import lax
from jax.experimental import pallas as pl
from jax.experimental.pallas import tpu as pltpu
from jax.sharding import PartitionSpec as P

HQ = 16
HK = 8
DH = 128
REACH = 2
GROUPS = HQ // HK
WIDTH = GROUPS * DH
TILE = 128
MASKED = -1e30

exponent_scale = 144.0 ** (-0.5) * math.log2(math.e)


LOG2E = math.log2(math.e)
SPLIT = HK // 2
MESH = pl.DeviceIdType.MESH


def kernel(
    shards,
    lengths_ref,
    queries_ref,
    keys_ref,
    values_ref,
    out_ref,
    held,
    query_held,
    out_held,
    query_back,
    slot,
    stat_out,
    stat_in,
    bias,
    back_bias,
    load_sem,
    query_sem,
    out_sem,
    core_send,
    core_recv,
    query_send,
    query_recv,
    slot_send,
    slot_recv,
    relay_send,
    relay_recv,
    stat_send,
    stat_recv,
):
    me = lax.axis_index("cp")
    core = lax.rem(me, 2)
    even = core == 0
    odd = core == 1
    partner = me + 1 - 2 * core
    rows = keys_ref.shape[0]
    docs = lengths_ref.shape[0]
    tiles = rows // TILE
    window = REACH * rows + TILE
    own = pl.ds(REACH * rows, rows)
    near = pl.ds(rows, rows)
    far = pl.ds(0, rows)
    has_prev = me >= 2
    has_next = me < shards - 2
    chip_begin = (me - core) * rows
    next_begin = chip_begin + 2 * rows

    def loads(head):
        lanes = pl.ds(pl.multiple_of(head * DH, DH), DH)
        return (
            pltpu.make_async_copy(keys_ref.at[:, lanes], held.at[head, 0, own], load_sem.at[head, 0]),
            pltpu.make_async_copy(values_ref.at[:, lanes], held.at[head, 1, own], load_sem.at[head, 1]),
        )

    def query_load(head):
        lanes = pl.ds(pl.multiple_of(head * WIDTH, WIDTH), WIDTH)
        return pltpu.make_async_copy(queries_ref.at[:, lanes], query_held.at[head], query_sem.at[head])

    def out_store(head):
        lanes = pl.ds(pl.multiple_of(head * WIDTH, WIDTH), WIDTH)
        return pltpu.make_async_copy(out_held.at[head], out_ref.at[:, lanes], out_sem.at[head])

    def remote(source, target, send, recv, device):
        return pltpu.make_async_remote_copy(
            src_ref=source,
            dst_ref=target,
            send_sem=send,
            recv_sem=recv,
            device_id={"cp": device},
            device_id_type=MESH,
        )

    def to_core(head, region):
        return remote(
            held.at[head, :, own], held.at[head, :, region], core_send.at[head], core_recv.at[head], partner
        )

    def query_to_prev(step, side):
        return remote(
            query_held.at[side * SPLIT + step],
            query_back.at[step],
            query_send.at[side * SPLIT + step],
            query_recv.at[step],
            me - 2 + side,
        )

    def slot_to_next(step, region):
        return remote(
            slot.at[step],
            held.at[core * SPLIT + step, :, region],
            slot_send.at[step],
            slot_recv.at[step],
            me + 2,
        )

    def relay(step, source, target):
        head = core * SPLIT + step
        return remote(
            held.at[head, :, source], held.at[head, :, target], relay_send.at[step], relay_recv.at[step], partner
        )

    def stat_to_next(step, head):
        return remote(
            stat_out.at[step], stat_in.at[head], stat_send.at[step], stat_recv.at[head], me + 2 - core
        )

    @pl.loop(0, SPLIT)
    def _(step):
        query_load(SPLIT + step).start()
        query_load(step).start()

    @pl.loop(0, HK)
    def _(head):
        for copy in loads(head):
            copy.start()

    barrier = pltpu.get_barrier_semaphore()

    def greet(device):
        pl.semaphore_signal(barrier, inc=1, device_id={"cp": device}, device_id_type=MESH)

    greet(partner)

    @pl.when(has_prev)
    def _():
        greet(me - 2)

        @pl.when(even)
        def _():
            greet(me - 1)

    @pl.when(has_next)
    def _():
        greet(me + 2)

        @pl.when(odd)
        def _():
            greet(me + 1)

    back_peers = jnp.where(has_prev, 2 - core, 0)
    next_peers = jnp.where(has_next, 1 + core, 0)
    pl.semaphore_wait(barrier, 1 + back_peers + next_peers)

    @pl.loop(0, SPLIT)
    def _(step):
        for side in (1, 0):
            query_load(side * SPLIT + step).wait()

            @pl.when(jnp.logical_and(even, has_prev))
            def _():
                query_to_prev(step, side).start()

    @pl.loop(0, HK)
    def _(head):
        for copy in loads(head):
            copy.wait()

        @pl.when(even)
        def _():
            to_core(head, near).start()

        @pl.when(jnp.logical_and(odd, head < SPLIT))
        def _():
            to_core(head, far).start()

    @pl.when(jnp.logical_not(has_prev))
    def _():
        @pl.when(even)
        def _():
            held[:, :, near, :] = jnp.zeros((HK, 2, rows, DH), held.dtype)
            stat_in[...] = jnp.full(stat_in.shape, MASKED, jnp.float32)

        @pl.when(odd)
        def _():
            held[:, :, far, :] = jnp.zeros((HK, 2, rows, DH), held.dtype)

    def doc_begins(positions):
        def next_doc(doc, state):
            end, begins = state
            end = end + lengths_ref[doc]
            return end, jnp.maximum(begins, jnp.where(positions >= end, end, 0))

        start = (jnp.int32(0), jnp.zeros(positions.shape, jnp.int32))
        return lax.fori_loop(0, docs, next_doc, start)[1]

    def sends_keys(boundary):
        positions = jnp.full((1, DH), boundary, jnp.int32)
        return boundary - doc_begins(positions) <= rows

    row_iota = lax.broadcasted_iota(jnp.int32, (TILE, 1), 0)
    floor = jnp.where(sends_keys(chip_begin), 0, chip_begin)[:, :1]
    for tile in range(tiles):
        query_pos = me * rows + tile * TILE + row_iota
        begins = jnp.maximum(doc_begins(query_pos), floor)
        first = jnp.where(even, (me - 1) * rows, (me - 2) * rows + tile * TILE)
        key_pos = first + lax.broadcasted_iota(jnp.int32, (TILE, window), 1)
        visible = (key_pos >= begins) & (key_pos <= query_pos)
        bias[pl.ds(tile * TILE, TILE), :] = jnp.where(visible, 0.0, MASKED)

    for tile in range(tiles):
        begins = doc_begins(next_begin + tile * TILE + row_iota)
        key_pos = chip_begin + lax.broadcasted_iota(jnp.int32, (TILE, 2 * rows), 1)
        back_bias[pl.ds(tile * TILE, TILE), :] = jnp.where(key_pos >= begins, 0.0, MASKED)

    next_keys = sends_keys(next_begin)
    diagonal = lax.broadcasted_iota(jnp.int32, (TILE, TILE), 0) == lax.broadcasted_iota(
        jnp.int32, (TILE, TILE), 1
    )

    def stack(queries):
        return jnp.concatenate([queries[:, g * DH : (g + 1) * DH] for g in range(GROUPS)], axis=0)

    def dot_keys(queries, keys):
        return lax.dot_general(
            queries, keys, (((1,), (1,)), ((), ())), preferred_element_type=jnp.float32
        )

    def softmax(scores, mask):
        scores = scores.reshape(GROUPS, TILE, scores.shape[-1]) * exponent_scale + mask[None]
        highest = jnp.max(scores, axis=-1, keepdims=True)
        weights = jnp.exp2(scores - highest)
        totals = jnp.sum(weights, axis=-1, keepdims=True)
        rounded = weights.astype(jnp.bfloat16).reshape(GROUPS * TILE, scores.shape[-1])
        return highest, totals, rounded

    def dot_values(weights, values):
        return jnp.dot(weights, values, preferred_element_type=jnp.float32)

    def attend_back(step):
        head = core * SPLIT + step
        older = pl.multiple_of((2 - core) * rows, TILE)
        newer = pl.multiple_of(2 * core * rows, TILE)
        newer_rows = pl.ds(newer, rows)
        for tile in range(tiles):
            span = pl.ds(tile * TILE, TILE)
            count = rows - tile * TILE
            older_rows = pl.ds(older + tile * TILE, count)
            queries = stack(query_back[step, span, :])
            scores = jnp.concatenate(
                [
                    dot_keys(queries, held[head, 0, older_rows, :]),
                    dot_keys(queries, held[head, 0, newer_rows, :]),
                ],
                axis=1,
            )
            highest, totals, weights = softmax(scores, back_bias[span, pl.ds(tile * TILE, count + rows)])
            mixed = dot_values(weights[:, :count], held[head, 1, older_rows, :]) + dot_values(
                weights[:, count:], held[head, 1, newer_rows, :]
            )
            mixed = mixed.reshape(GROUPS, TILE, DH) / totals
            level = highest + jnp.log(totals) * LOG2E
            sent = pl.ds(newer + tile * TILE, TILE)
            for g in range(GROUPS):
                kept = held[head, g, sent, :].astype(jnp.float32)
                slot[step, g, span, :] = jnp.where(next_keys, kept, mixed[g]).astype(jnp.bfloat16)
                row = jnp.sum(jnp.where(diagonal, level[g], 0.0), axis=0, keepdims=True)
                stat_out[step, pl.ds(tile * GROUPS + g, 1), :] = jnp.where(next_keys, MASKED, row)

    def attend_even(head):
        for tile in range(tiles):
            span = pl.ds(tile * TILE, TILE)
            count = rows + (tile + 1) * TILE
            keys = pl.ds(rows, count)
            scores = dot_keys(stack(query_held[head, span, :]), held[head, 0, keys, :])
            highest, totals, weights = softmax(scores, bias[span, pl.ds(0, count)])
            mixed = dot_values(weights, held[head, 1, keys, :]).reshape(GROUPS, TILE, DH)
            for g in range(GROUPS):
                row = stat_in[head, pl.ds(tile * GROUPS + g, 1), :]
                level = jnp.sum(jnp.where(diagonal, row, 0.0), axis=1, keepdims=True)
                top = jnp.maximum(highest[g], level)
                here = jnp.exp2(highest[g] - top)
                there = jnp.exp2(level - top)
                partial = held[head, g, pl.ds(rows + tile * TILE, TILE), :].astype(jnp.float32)
                both = (mixed[g] * here + partial * there) / (totals[g] * here + there)
                out_held[head, span, pl.ds(g * DH, DH)] = both.astype(jnp.bfloat16)

    def attend_odd(head):
        for tile in range(tiles):
            span = pl.ds(tile * TILE, TILE)
            keys = pl.ds(tile * TILE, window)
            scores = dot_keys(stack(query_held[head, span, :]), held[head, 0, keys, :])
            _, totals, weights = softmax(scores, bias[span, :])
            mixed = dot_values(weights, held[head, 1, keys, :]).reshape(GROUPS, TILE, DH)
            mixed = (mixed / totals).astype(jnp.bfloat16)
            for g in range(GROUPS):
                out_held[head, span, pl.ds(g * DH, DH)] = mixed[g]

    @pl.when(even)
    def _():
        @pl.loop(0, SPLIT)
        def _(head):
            to_core(head, far).wait_recv()

    @pl.when(odd)
    def _():
        @pl.loop(0, HK)
        def _(head):
            to_core(head, near).wait_recv()

    @pl.loop(0, SPLIT + 1)
    def _(turn):
        @pl.when(jnp.logical_and(has_next, turn < SPLIT))
        def _():
            query_to_prev(turn, 0).wait_recv()
            attend_back(turn)

            @pl.when(even)
            def _():
                slot_to_next(turn, near).start()

            @pl.when(odd)
            def _():
                slot_to_next(turn, far).start()

            stat_to_next(turn, core * SPLIT + turn).start()

        @pl.when(turn >= 1)
        def _():
            step = turn - 1

            @pl.when(has_prev)
            def _():
                slot_to_next(step, far).wait_recv()

                @pl.when(even)
                def _():
                    relay(step, near, far).start()

                @pl.when(odd)
                def _():
                    relay(step, far, near).start()

            @pl.loop(0, 2)
            def _(turn_side):
                side = lax.rem(core + turn_side, 2)
                head = side * SPLIT + step

                @pl.when(jnp.logical_and(has_prev, turn_side == 1))
                def _():
                    relay(step, near, far).wait_recv()

                @pl.when(even)
                def _():
                    @pl.when(has_prev)
                    def _():
                        stat_to_next(step, head).wait_recv()

                    attend_even(head)

                @pl.when(odd)
                def _():
                    attend_odd(head)

                out_store(head).start()

    @pl.loop(0, HK)
    def _(head):
        out_store(head).wait()

        @pl.when(jnp.logical_or(even, head < SPLIT))
        def _():
            to_core(head, near).wait_send()

    @pl.loop(0, SPLIT)
    def _(step):
        @pl.when(has_next)
        def _():
            slot_to_next(step, near).wait_send()
            stat_to_next(step, step).wait_send()

        @pl.when(has_prev)
        def _():
            relay(step, near, far).wait_send()

            @pl.when(even)
            def _():
                for side in range(2):
                    query_to_prev(step, side).wait_send()


def on_device(queries, keys, values, doc_lengths):
    rows = keys.shape[0]
    shards = lax.axis_size("cp")
    window = REACH * rows + TILE
    stats = rows // TILE * GROUPS
    dma = pltpu.SemaphoreType.DMA
    return pl.pallas_call(
        functools.partial(kernel, shards),
        out_shape=jax.ShapeDtypeStruct(queries.shape, queries.dtype),
        in_specs=[
            pl.BlockSpec(memory_space=pltpu.SMEM),
            pl.BlockSpec(memory_space=pl.ANY),
            pl.BlockSpec(memory_space=pl.ANY),
            pl.BlockSpec(memory_space=pl.ANY),
        ],
        out_specs=pl.BlockSpec(memory_space=pl.ANY),
        scratch_shapes=[
            pltpu.VMEM((HK, 2, (REACH + 1) * rows, DH), keys.dtype),
            pltpu.VMEM((HK, rows, WIDTH), queries.dtype),
            pltpu.VMEM((HK, rows, WIDTH), queries.dtype),
            pltpu.VMEM((SPLIT, rows, WIDTH), queries.dtype),
            pltpu.VMEM((SPLIT, 2, rows, DH), keys.dtype),
            pltpu.VMEM((SPLIT, stats, TILE), jnp.float32),
            pltpu.VMEM((HK, stats, TILE), jnp.float32),
            pltpu.VMEM((rows, window), jnp.float32),
            pltpu.VMEM((rows, REACH * rows), jnp.float32),
            dma((HK, 2)),
            dma((HK,)),
            dma((HK,)),
            dma((HK,)),
            dma((HK,)),
            dma((HK,)),
            dma((SPLIT,)),
            dma((SPLIT,)),
            dma((SPLIT,)),
            dma((SPLIT,)),
            dma((SPLIT,)),
            dma((SPLIT,)),
            dma((HK,)),
        ],
        compiler_params=pltpu.CompilerParams(
            collective_id=0, has_side_effects=True, vmem_limit_bytes=58 * 1024 * 1024
        ),
    )(doc_lengths, queries, keys, values)


def solution(mesh):
    return jax.shard_map(
        on_device,
        mesh=mesh,
        in_specs=(P(("grp", "cp"), None), P(("grp", "cp"), None), P(("grp", "cp"), None), P("grp")),
        out_specs=P(("grp", "cp"), None),
        check_vma=False,
    )
```
